32 devices in a mesh: gx: 4 (over y, x), gy: 2 (over core), gz: 4 (over z).
Axes of the slice: x: 2, y: 2, z: 4, core: 2. Of those that a mesh axis runs over, the one named last changes fastest.
Arguments:
- flow_state: float32 [6, 16, 32, 512], P(None, 'gx', 'gy', 'gz'), may hold values from -6 to 6
Outputs:
- new_vorticity: float32 [3, 16, 32, 512], P(None, 'gx', 'gy', 'gz')
The draws below stay inside these ranges and needn't reach their ends.
All inputs are finite; a program needn't handle non-finite values.
Results may differ from the reference program's by a relative error of at most 0.0001.
Values sent between devices are 32-bit elements; how exact they have to be, the bound alone decides.
A program may use at most 64 MiB of HBM per device.

```python
import jax
import jax.numpy as jnp
from jax import lax

NX = 16
NY = 32
NZ = 512


def block_scale(rng, extent, cuts, smallest, top_value):
    loudness = 1.0
    for axis_at, shards_of in cuts:
        steps = jax.random.uniform(jax.random.fold_in(jax.random.fold_in(rng, 6), axis_at), (shards_of,), jnp.float32, smallest / len(cuts), top_value / len(cuts))
        loudness = loudness * jnp.repeat(jnp.exp(steps), extent[axis_at] // shards_of).reshape((-1,) + (1,) * (len(extent) - 1 - axis_at))
    return loudness


def gaussian(rng, extent, scale, reach, cuts=(), kind=jnp.bfloat16):
    result = scale * jax.random.normal(rng, extent, jnp.float32)
    if cuts:
        result = result * block_scale(rng, extent, cuts, -0.22, 0.18)
    return jnp.clip(result, -reach, reach).astype(kind)


def setup_inputs(seed: int = 0) -> dict:
    seeds = jax.random.split(jax.random.key(seed), 2)
    return {
        "flow_state": gaussian(seeds[0], (6, NX, NY, NZ), 1.0, 6.0, ((1, 4), (2, 2), (3, 4)), jnp.float32),
    }


def derivatives(values, dimension):
    minus_two = jnp.roll(values, 2, axis=dimension)
    minus_one = jnp.roll(values, 1, axis=dimension)
    plus_one = jnp.roll(values, -1, axis=dimension)
    plus_two = jnp.roll(values, -2, axis=dimension)
    gradient = (8.0 * (plus_one - minus_one) - (plus_two - minus_two)) / 12.0
    curvature = (16.0 * (plus_one + minus_one) - (plus_two + minus_two) - 30.0 * values) / 12.0
    return (gradient, curvature)

def reference(flow_state):
    vorticity = flow_state[0:3]
    velocity = flow_state[3:6]
    gradients = []
    laplace = jnp.zeros_like(vorticity)
    for dimension in range(3):
        gradient, unused = derivatives(velocity, dimension + 1)
        unused_grad, curvature = derivatives(vorticity, dimension + 1)
        gradients.append(gradient)
        laplace = laplace + curvature
    strain = jnp.zeros(vorticity.shape[1:], jnp.float32)
    for gradient in gradients:
        strain = strain + lax.optimization_barrier(jnp.sum(gradient * gradient, axis=0))
    peak = jnp.max(strain)
    step_size = 0.25 / jnp.maximum(1.0, jnp.sqrt(peak))
    stretch = jnp.zeros_like(vorticity)
    for dimension in range(3):
        stretch = stretch + vorticity[dimension:dimension + 1] * gradients[dimension]
    return vorticity + step_size * (stretch + 0.5 * laplace)
```

```python
import functools

import jax
import jax.numpy as jnp
from jax import lax
from jax.experimental import pallas as pl
from jax.experimental.pallas import tpu as pltpu
from jax.sharding import PartitionSpec as P

MESH = pl.DeviceIdType.MESH
AXES = ("gx", "gy", "gz")
LANES = 4


def shifted(values, side, dim):
    length = values.shape[dim]
    index = lax.broadcasted_iota(jnp.int32, values.shape, dim)
    return (
        pltpu.roll(jnp.where(index >= length - 2, side, values), 2, dim),
        pltpu.roll(jnp.where(index >= length - 1, side, values), 1, dim),
        pltpu.roll(jnp.where(index < 1, side, values), length - 1, dim),
        pltpu.roll(jnp.where(index < 2, side, values), length - 2, dim),
    )


def gradient(m2, m1, p1, p2):
    return (8.0 * (p1 - m1) - (p2 - m2)) * (1.0 / 12.0)


def curvature(m2, m1, center, p1, p2):
    return (16.0 * (p1 + m1) - (p2 + m2) - 30.0 * center) * (1.0 / 12.0)


def kernel(
    counts,
    flow_ref,
    out_ref,
    state,
    packed,
    from_down,
    from_up,
    beside,
    left,
    right,
    strain_ref,
    plane_peaks,
    line_peaks,
    load_sem,
    halo_send,
    halo_recv,
    plane_send,
    plane_recv,
    line_send,
    line_recv,
):
    nx, ny, nz = counts
    components, depth, rows, lanes = state.shape
    half = components // 2
    me = [lax.axis_index(axis) for axis in AXES]

    def peer(dx, dy, dz):
        return tuple(
            lax.rem(at + (step % count), count) for at, step, count in zip(me, (dx, dy, dz), counts)
        )

    plane = [(dx, dy, 0) for dx in range(nx) for dy in range(ny) if (dx, dy) != (0, 0)]
    line = [(0, 0, dz) for dz in range(1, nz)]

    loads = [
        pltpu.make_async_copy(flow_ref.at[part], state.at[part], load_sem.at[i])
        for i, part in enumerate((pl.ds(half, half), pl.ds(0, half)))
    ]
    for load in loads:
        load.start()
    barrier = pltpu.get_barrier_semaphore()
    for offset in plane + line:
        pl.semaphore_signal(barrier, inc=1, device_id=peer(*offset), device_id_type=MESH)

    for load in loads:
        load.wait()
    tiles = [(c, x) for c in range(components) for x in range(depth)]
    per_pack = lanes // LANES
    lane = lax.broadcasted_iota(jnp.int32, (rows, lanes), 1)
    for p in range(packed.shape[0]):
        total = jnp.zeros((rows, lanes), jnp.float32)
        for t, (c, x) in enumerate(tiles[p * per_pack : (p + 1) * per_pack]):
            moved = pltpu.roll(state[c, x], (LANES * t + 2) % lanes, 1)
            total = jnp.where(lane >= LANES * t, moved, total)
        packed[p] = total

    pl.semaphore_wait(barrier, len(plane) + len(line))

    def send(i, source, target, offset):
        copy = pltpu.make_async_remote_copy(
            src_ref=source,
            dst_ref=target,
            send_sem=halo_send.at[i],
            recv_sem=halo_recv.at[i],
            device_id=peer(*offset),
            device_id_type=MESH,
        )
        copy.start()
        return copy

    velocity, vorticity = pl.ds(half, half), pl.ds(0, half)
    u_copies = [
        send(0, state.at[velocity, pl.ds(depth - 2, 2)], left.at[velocity], (1, 0, 0)),
        send(1, state.at[velocity, pl.ds(0, 2)], right.at[velocity], (-1, 0, 0)),
    ]
    near_copies = [
        send(2, packed, from_down, (0, 0, 1)),
        send(3, packed, from_up, (0, 0, -1)),
        send(4, state.at[:, :, pl.ds(rows - 8, 8)], beside.at[:, :, pl.ds(rows - 8, 8)], (0, 1, 0)),
        send(5, state.at[:, :, pl.ds(0, 8)], beside.at[:, :, pl.ds(0, 8)], (0, -1, 0)),
    ]
    w_copies = [
        send(6, state.at[vorticity, pl.ds(depth - 2, 2)], left.at[vorticity], (1, 0, 0)),
        send(7, state.at[vorticity, pl.ds(0, 2)], right.at[vorticity], (-1, 0, 0)),
    ]

    for copy in near_copies:
        copy.wait_recv()
    sides = [
        jnp.where((lane % LANES) < 2, from_down[p], from_up[p]) for p in range(packed.shape[0])
    ]

    def z_side(c, x):
        t = c * depth + x
        return pltpu.roll(sides[t // per_pack], (lanes - (LANES * (t % per_pack) + 2)) % lanes, 1)

    for x in range(depth):
        strain = jnp.zeros((rows, lanes), jnp.float32)
        w_y, w_z = state[1, x], state[2, x]
        for c in range(half):
            u, w = state[half + c, x], state[c, x]
            grad_y = gradient(*shifted(u, beside[half + c, x], 0))
            grad_z = gradient(*shifted(u, z_side(half + c, x), 1))
            strain = strain + grad_y * grad_y + grad_z * grad_z
            m2, m1, p1, p2 = shifted(w, beside[c, x], 0)
            laplace = curvature(m2, m1, w, p1, p2)
            m2, m1, p1, p2 = shifted(w, z_side(c, x), 1)
            laplace = laplace + curvature(m2, m1, w, p1, p2)
            out_ref[c, x] = w_y * grad_y + w_z * grad_z + 0.5 * laplace
        strain_ref[x] = strain

    def layer(c, x):
        if x < 0:
            return left[c, x + 2]
        if x >= depth:
            return right[c, x - depth]
        return state[c, x]

    for copy in u_copies:
        copy.wait_recv()
    peak = jnp.zeros((rows, lanes), jnp.float32)
    for x in range(depth):
        strain = strain_ref[x]
        w_x = state[0, x]
        for c in range(half):
            grad_x = gradient(*(layer(half + c, x + k) for k in (-2, -1, 1, 2)))
            strain = strain + grad_x * grad_x
            out_ref[c, x] = out_ref[c, x] + w_x * grad_x
        peak = jnp.maximum(peak, strain)

    def spread(values, slots, offsets, send_sem, recv_sem):
        slots[0] = values
        copies = []
        for i, offset in enumerate(offsets):
            copy = pltpu.make_async_remote_copy(
                src_ref=slots.at[0],
                dst_ref=slots.at[i + 1],
                send_sem=send_sem.at[i],
                recv_sem=recv_sem.at[i],
                device_id=peer(*offset),
                device_id_type=MESH,
            )
            copy.start()
            copies.append(copy)
        return copies

    peak_copies = spread(
        jnp.max(peak, axis=0, keepdims=True), plane_peaks, plane, plane_send, plane_recv
    )
    for copy in w_copies:
        copy.wait_recv()
    for x in range(depth):
        for c in range(half):
            m2, m1, w, p1, p2 = (layer(c, x + k) for k in (-2, -1, 0, 1, 2))
            out_ref[c, x] = out_ref[c, x] + 0.5 * curvature(m2, m1, w, p1, p2)
    for copy in peak_copies:
        copy.wait_recv()
    line_copies = spread(
        jnp.max(plane_peaks[...], axis=0), line_peaks, line, line_send, line_recv
    )
    for copy in line_copies:
        copy.wait_recv()
    peak = jnp.max(jnp.max(line_peaks[...], axis=0), axis=1, keepdims=True)
    step_size = 0.25 / jnp.maximum(1.0, jnp.sqrt(peak))
    for x in range(depth):
        for c in range(half):
            out_ref[c, x] = state[c, x] + step_size * out_ref[c, x]
    for copy in u_copies + near_copies + w_copies + peak_copies + line_copies:
        copy.wait_send()


def on_device(counts, flow_state):
    components, depth, rows, lanes = flow_state.shape
    nx, ny, nz = counts
    half = components // 2
    per_pack = lanes // LANES
    packs = -(-components * depth // per_pack)
    plane, line = nx * ny - 1, nz - 1
    f32 = jnp.float32
    dma = pltpu.SemaphoreType.DMA
    return pl.pallas_call(
        functools.partial(kernel, counts),
        out_shape=jax.ShapeDtypeStruct((half, depth, rows, lanes), f32),
        in_specs=[pl.BlockSpec(memory_space=pl.ANY)],
        out_specs=pl.BlockSpec(memory_space=pltpu.VMEM),
        scratch_shapes=[
            pltpu.VMEM((components, depth, rows, lanes), f32),
            pltpu.VMEM((packs, rows, lanes), f32),
            pltpu.VMEM((packs, rows, lanes), f32),
            pltpu.VMEM((packs, rows, lanes), f32),
            pltpu.VMEM((components, depth, rows, lanes), f32),
            pltpu.VMEM((components, 2, rows, lanes), f32),
            pltpu.VMEM((components, 2, rows, lanes), f32),
            pltpu.VMEM((depth, rows, lanes), f32),
            pltpu.VMEM((plane + 1, 1, lanes), f32),
            pltpu.VMEM((line + 1, 1, lanes), f32),
            dma((2,)),
            dma((8,)),
            dma((8,)),
            dma((plane,)),
            dma((plane,)),
            dma((line,)),
            dma((line,)),
        ],
        compiler_params=pltpu.CompilerParams(collective_id=0, has_side_effects=True),
    )(flow_state)


def solution(mesh):
    counts = tuple(mesh.shape[axis] for axis in AXES)
    return jax.shard_map(
        functools.partial(on_device, counts),
        mesh=mesh,
        in_specs=(P(None, *AXES),),
        out_specs=P(None, *AXES),
        check_vma=False,
    )
```

```python
import functools

import jax
import jax.numpy as jnp
from jax import lax
from jax.experimental import pallas as pl
from jax.experimental.pallas import tpu as pltpu
from jax.sharding import PartitionSpec as P

MESH = pl.DeviceIdType.MESH
AXES = ("gx", "gy", "gz")
LANES = 4
VMEM_BYTES = 4 * 1024 * 1024


def shifted(values, side, dim):
    length = values.shape[dim]
    index = lax.broadcasted_iota(jnp.int32, values.shape, dim)
    return (
        pltpu.roll(jnp.where(index >= length - 2, side, values), 2, dim),
        pltpu.roll(jnp.where(index >= length - 1, side, values), 1, dim),
        pltpu.roll(jnp.where(index < 1, side, values), length - 1, dim),
        pltpu.roll(jnp.where(index < 2, side, values), length - 2, dim),
    )


def gradient(m2, m1, p1, p2):
    return (8.0 * (p1 - m1) - (p2 - m2)) * (1.0 / 12.0)


def curvature(m2, m1, center, p1, p2):
    return (16.0 * (p1 + m1) - (p2 + m2) - 30.0 * center) * (1.0 / 12.0)


def kernel(
    counts,
    flow_ref,
    out_ref,
    state,
    packed,
    from_down,
    from_up,
    beside,
    left,
    right,
    strain_ref,
    peaks,
    load_sem,
    halo_send,
    halo_recv,
    peak_send,
    peak_recv,
    ready,
):
    nx, ny, nz = counts
    components, depth, rows, lanes = state.shape
    half = components // 2
    me = [lax.axis_index(axis) for axis in AXES]

    def peer(dx, dy, dz):
        return tuple(
            lax.rem(at + (step % count), count) for at, step, count in zip(me, (dx, dy, dz), counts)
        )

    plane = [(dx, dy, 0) for dx in range(nx) for dy in range(ny) if (dx, dy) != (0, 0)]
    line = [(0, 0, dz) for dz in range(1, nz)]
    others = [(dx, dy, dz) for dz in range(1, nz) for dx in range(nx) for dy in range(ny)] + plane

    loads = [
        pltpu.make_async_copy(flow_ref.at[part], state.at[part], load_sem.at[i])
        for i, part in enumerate((pl.ds(half, half), pl.ds(0, half)))
    ]
    barrier = pltpu.get_barrier_semaphore()
    for offset in line + plane:
        pl.semaphore_signal(barrier, inc=1, device_id=peer(*offset), device_id_type=MESH)
    for load in loads:
        load.start()

    for load in loads:
        load.wait()
    tiles = [(c, x) for c in range(components) for x in range(depth)]
    per_pack = lanes // LANES
    lane = lax.broadcasted_iota(jnp.int32, (rows, lanes), 1)
    for p in range(packed.shape[0]):
        total = jnp.zeros((rows, lanes), jnp.float32)
        for t, (c, x) in enumerate(tiles[p * per_pack : (p + 1) * per_pack]):
            moved = pltpu.roll(state[c, x], (LANES * t + 2) % lanes, 1)
            total = jnp.where(lane >= LANES * t, moved, total)
        packed[p] = total

    pl.semaphore_wait(barrier, len(plane) + len(line))

    def send(i, source, target, offset):
        copy = pltpu.make_async_remote_copy(
            src_ref=source,
            dst_ref=target,
            send_sem=halo_send.at[i],
            recv_sem=halo_recv.at[i],
            device_id=peer(*offset),
            device_id_type=MESH,
        )
        copy.start()
        return copy

    velocity, vorticity = pl.ds(half, half), pl.ds(0, half)
    u_copies = [
        send(0, state.at[velocity, pl.ds(depth - 2, 2)], left.at[velocity], (1, 0, 0)),
        send(1, state.at[velocity, pl.ds(0, 2)], right.at[velocity], (-1, 0, 0)),
    ]
    near_copies = [
        send(2, packed, from_down, (0, 0, 1)),
        send(3, packed, from_up, (0, 0, -1)),
        send(4, state.at[:, :, pl.ds(rows - 8, 8)], beside.at[:, :, pl.ds(rows - 8, 8)], (0, 1, 0)),
        send(5, state.at[:, :, pl.ds(0, 8)], beside.at[:, :, pl.ds(0, 8)], (0, -1, 0)),
    ]
    w_copies = [
        send(6, state.at[vorticity, pl.ds(depth - 2, 2)], left.at[vorticity], (1, 0, 0)),
        send(7, state.at[vorticity, pl.ds(0, 2)], right.at[vorticity], (-1, 0, 0)),
    ]

    for offset in plane:
        pl.semaphore_signal(ready, inc=1, device_id=peer(*offset), device_id_type=MESH)

    for copy in near_copies:
        copy.wait_recv()
    sides = [
        jnp.where((lane % LANES) < 2, from_down[p], from_up[p]) for p in range(packed.shape[0])
    ]

    def z_side(c, x):
        t = c * depth + x
        return pltpu.roll(sides[t // per_pack], (lanes - (LANES * (t % per_pack) + 2)) % lanes, 1)

    for x in range(depth):
        strain = jnp.zeros((rows, lanes), jnp.float32)
        w_y, w_z = state[1, x], state[2, x]
        for c in range(half):
            u, w = state[half + c, x], state[c, x]
            grad_y = gradient(*shifted(u, beside[half + c, x], 0))
            grad_z = gradient(*shifted(u, z_side(half + c, x), 1))
            strain = strain + grad_y * grad_y + grad_z * grad_z
            m2, m1, p1, p2 = shifted(w, beside[c, x], 0)
            laplace = curvature(m2, m1, w, p1, p2)
            m2, m1, p1, p2 = shifted(w, z_side(c, x), 1)
            laplace = laplace + curvature(m2, m1, w, p1, p2)
            out_ref[c, x] = w_y * grad_y + w_z * grad_z + 0.5 * laplace
        strain_ref[x] = strain

    def layer(c, x):
        if x < 0:
            return left[c, x + 2]
        if x >= depth:
            return right[c, x - depth]
        return state[c, x]

    for copy in u_copies:
        copy.wait_recv()
    peak = jnp.zeros((rows, lanes), jnp.float32)
    for x in range(depth):
        strain = strain_ref[x]
        w_x = state[0, x]
        for c in range(half):
            grad_x = gradient(*(layer(half + c, x + k) for k in (-2, -1, 1, 2)))
            strain = strain + grad_x * grad_x
            out_ref[c, x] = out_ref[c, x] + w_x * grad_x
        peak = jnp.maximum(peak, strain)

    peaks[0] = jnp.max(peak, axis=0, keepdims=True)
    pl.semaphore_wait(ready, len(plane))
    peak_copies = []
    for i, offset in enumerate(others):
        copy = pltpu.make_async_remote_copy(
            src_ref=peaks.at[0],
            dst_ref=peaks.at[i + 1],
            send_sem=peak_send,
            recv_sem=peak_recv,
            device_id=peer(*offset),
            device_id_type=MESH,
        )
        copy.start()
        peak_copies.append(copy)
    for copy in w_copies:
        copy.wait_recv()
    for x in range(depth):
        for c in range(half):
            m2, m1, w, p1, p2 = (layer(c, x + k) for k in (-2, -1, 0, 1, 2))
            out_ref[c, x] = out_ref[c, x] + 0.5 * curvature(m2, m1, w, p1, p2)
    pltpu.make_async_copy(peaks.at[pl.ds(1, len(others))], peaks.at[pl.ds(1, len(others))], peak_send).wait()
    for copy in u_copies + near_copies + w_copies:
        copy.wait_send()
    everyone = pltpu.make_async_copy(peaks.at[pl.ds(1, len(others))], peaks.at[pl.ds(1, len(others))], peak_recv)
    everyone.wait()
    peak = jnp.max(jnp.max(peaks[...], axis=0), axis=1, keepdims=True)
    step_size = 0.25 / jnp.maximum(1.0, jnp.sqrt(peak))
    for x in range(depth):
        for c in range(half):
            out_ref[c, x] = state[c, x] + step_size * out_ref[c, x]


def on_device(counts, flow_state):
    components, depth, rows, lanes = flow_state.shape
    nx, ny, nz = counts
    half = components // 2
    per_pack = lanes // LANES
    packs = -(-components * depth // per_pack)
    devices = nx * ny * nz
    f32 = jnp.float32
    dma = pltpu.SemaphoreType.DMA
    return pl.pallas_call(
        functools.partial(kernel, counts),
        out_shape=jax.ShapeDtypeStruct((half, depth, rows, lanes), f32),
        in_specs=[pl.BlockSpec(memory_space=pl.ANY)],
        out_specs=pl.BlockSpec(memory_space=pltpu.VMEM),
        scratch_shapes=[
            pltpu.VMEM((components, depth, rows, lanes), f32),
            pltpu.VMEM((packs, rows, lanes), f32),
            pltpu.VMEM((packs, rows, lanes), f32),
            pltpu.VMEM((packs, rows, lanes), f32),
            pltpu.VMEM((components, depth, rows, lanes), f32),
            pltpu.VMEM((components, 2, rows, lanes), f32),
            pltpu.VMEM((components, 2, rows, lanes), f32),
            pltpu.VMEM((depth, rows, lanes), f32),
            pltpu.VMEM((devices, 1, lanes), f32),
            dma((2,)),
            dma((8,)),
            dma((8,)),
            dma,
            dma,
            pltpu.SemaphoreType.REGULAR,
        ],
        compiler_params=pltpu.CompilerParams(collective_id=0, has_side_effects=True, vmem_limit_bytes=VMEM_BYTES),
    )(flow_state)


def solution(mesh):
    counts = tuple(mesh.shape[axis] for axis in AXES)
    return jax.shard_map(
        functools.partial(on_device, counts),
        mesh=mesh,
        in_specs=(P(None, *AXES),),
        out_specs=P(None, *AXES),
        check_vma=False,
    )
```

```python
import functools

import jax
import jax.numpy as jnp
from jax import lax
from jax.experimental import pallas as pl
from jax.experimental.pallas import tpu as pltpu
from jax.sharding import PartitionSpec as P

MESH = pl.DeviceIdType.MESH
AXES = ("gx", "gy", "gz")
LANES = 4
VMEM_BYTES = 4 * 1024 * 1024


def shifted(values, side, dim):
    length = values.shape[dim]
    index = lax.broadcasted_iota(jnp.int32, values.shape, dim)
    return (
        pltpu.roll(jnp.where(index >= length - 2, side, values), 2, dim),
        pltpu.roll(jnp.where(index >= length - 1, side, values), 1, dim),
        pltpu.roll(jnp.where(index < 1, side, values), length - 1, dim),
        pltpu.roll(jnp.where(index < 2, side, values), length - 2, dim),
    )


def gradient(m2, m1, p1, p2):
    return (8.0 * (p1 - m1) - (p2 - m2)) * (1.0 / 12.0)


def curvature(m2, m1, center, p1, p2):
    return (16.0 * (p1 + m1) - (p2 + m2) - 30.0 * center) * (1.0 / 12.0)


def kernel(
    counts,
    flow_ref,
    out_ref,
    state,
    packed,
    from_down,
    from_up,
    beside,
    left,
    right,
    strain_ref,
    peaks,
    load_sem,
    halo_send,
    halo_recv,
    peak_send,
    peak_recv,
    ready,
):
    nx, ny, nz = counts
    components, depth, rows, lanes = state.shape
    half = components // 2
    me = [lax.axis_index(axis) for axis in AXES]

    def peer(dx, dy, dz):
        return tuple(
            lax.rem(at + (step % count), count) for at, step, count in zip(me, (dx, dy, dz), counts)
        )

    plane = [(dx, dy, 0) for dx in range(nx) for dy in range(ny) if (dx, dy) != (0, 0)]
    line = [(0, 0, dz) for dz in range(1, nz)]
    others = [(dx, dy, dz) for dz in range(1, nz) for dx in range(nx) for dy in range(ny)] + plane

    loads = [
        pltpu.make_async_copy(flow_ref.at[part], state.at[part], load_sem.at[i])
        for i, part in enumerate((pl.ds(half, half), pl.ds(0, half)))
    ]
    barrier = pltpu.get_barrier_semaphore()
    for offset in line + plane:
        pl.semaphore_signal(barrier, inc=1, device_id=peer(*offset), device_id_type=MESH)
    for load in loads:
        load.start()

    for load in loads:
        load.wait()
    tiles = [(c, x) for c in range(components) for x in range(depth)]
    per_pack = lanes // LANES
    lane = lax.broadcasted_iota(jnp.int32, (rows, lanes), 1)
    for p in range(packed.shape[0]):
        total = jnp.zeros((rows, lanes), jnp.float32)
        for t, (c, x) in enumerate(tiles[p * per_pack : (p + 1) * per_pack]):
            moved = pltpu.roll(state[c, x], (LANES * t + 2) % lanes, 1)
            total = jnp.where(lane >= LANES * t, moved, total)
        packed[p] = total

    pl.semaphore_wait(barrier, len(plane) + len(line))

    def send(i, source, target, offset):
        copy = pltpu.make_async_remote_copy(
            src_ref=source,
            dst_ref=target,
            send_sem=halo_send.at[i],
            recv_sem=halo_recv.at[i],
            device_id=peer(*offset),
            device_id_type=MESH,
        )
        copy.start()
        return copy

    velocity, vorticity = pl.ds(half, half), pl.ds(0, half)
    u_copies = [
        send(0, state.at[velocity, pl.ds(depth - 2, 2)], left.at[velocity], (1, 0, 0)),
        send(1, state.at[velocity, pl.ds(0, 2)], right.at[velocity], (-1, 0, 0)),
    ]
    near_copies = [
        send(2, packed, from_down, (0, 0, 1)),
        send(3, packed, from_up, (0, 0, -1)),
        send(4, state.at[:, :, pl.ds(rows - 8, 8)], beside.at[:, :, pl.ds(rows - 8, 8)], (0, 1, 0)),
        send(5, state.at[:, :, pl.ds(0, 8)], beside.at[:, :, pl.ds(0, 8)], (0, -1, 0)),
    ]
    for offset in plane:
        pl.semaphore_signal(ready, inc=1, device_id=peer(*offset), device_id_type=MESH)

    for copy in near_copies:
        copy.wait_recv()
    sides = [
        jnp.where((lane % LANES) < 2, from_down[p], from_up[p]) for p in range(packed.shape[0])
    ]

    def z_side(c, x):
        t = c * depth + x
        return pltpu.roll(sides[t // per_pack], (lanes - (LANES * (t % per_pack) + 2)) % lanes, 1)

    for x in range(depth):
        strain = jnp.zeros((rows, lanes), jnp.float32)
        w_y, w_z = state[1, x], state[2, x]
        for c in range(half):
            u = state[half + c, x]
            grad_y = gradient(*shifted(u, beside[half + c, x], 0))
            grad_z = gradient(*shifted(u, z_side(half + c, x), 1))
            strain = strain + grad_y * grad_y + grad_z * grad_z
            out_ref[c, x] = w_y * grad_y + w_z * grad_z
        strain_ref[x] = strain

    def layer(c, x):
        if x < 0:
            return left[c, x + 2]
        if x >= depth:
            return right[c, x - depth]
        return state[c, x]

    for copy in u_copies:
        copy.wait_recv()
    peak = jnp.zeros((rows, lanes), jnp.float32)
    for x in range(depth):
        strain = strain_ref[x]
        w_x = state[0, x]
        for c in range(half):
            grad_x = gradient(*(layer(half + c, x + k) for k in (-2, -1, 1, 2)))
            strain = strain + grad_x * grad_x
            out_ref[c, x] = out_ref[c, x] + w_x * grad_x
        peak = jnp.maximum(peak, strain)

    peaks[0] = jnp.max(peak, axis=0, keepdims=True)
    pl.semaphore_wait(ready, len(plane))
    peak_copies = []
    for i, offset in enumerate(others):
        copy = pltpu.make_async_remote_copy(
            src_ref=peaks.at[0],
            dst_ref=peaks.at[i + 1],
            send_sem=peak_send,
            recv_sem=peak_recv,
            device_id=peer(*offset),
            device_id_type=MESH,
        )
        copy.start()
        peak_copies.append(copy)
    w_copies = [
        send(6, state.at[vorticity, pl.ds(depth - 2, 2)], left.at[vorticity], (1, 0, 0)),
        send(7, state.at[vorticity, pl.ds(0, 2)], right.at[vorticity], (-1, 0, 0)),
    ]
    for copy in w_copies:
        copy.wait_recv()
    for x in range(depth):
        for c in range(half):
            m2, m1, w, p1, p2 = (layer(c, x + k) for k in (-2, -1, 0, 1, 2))
            laplace = curvature(m2, m1, w, p1, p2)
            m2, m1, p1, p2 = shifted(w, beside[c, x], 0)
            laplace = laplace + curvature(m2, m1, w, p1, p2)
            m2, m1, p1, p2 = shifted(w, z_side(c, x), 1)
            laplace = laplace + curvature(m2, m1, w, p1, p2)
            out_ref[c, x] = out_ref[c, x] + 0.5 * laplace
    pltpu.make_async_copy(peaks.at[pl.ds(1, len(others))], peaks.at[pl.ds(1, len(others))], peak_send).wait()
    for copy in u_copies + near_copies + w_copies:
        copy.wait_send()
    everyone = pltpu.make_async_copy(peaks.at[pl.ds(1, len(others))], peaks.at[pl.ds(1, len(others))], peak_recv)
    everyone.wait()
    peak = jnp.max(jnp.max(peaks[...], axis=0), axis=1, keepdims=True)
    step_size = 0.25 / jnp.maximum(1.0, jnp.sqrt(peak))
    for x in range(depth):
        for c in range(half):
            out_ref[c, x] = state[c, x] + step_size * out_ref[c, x]


def on_device(counts, flow_state):
    components, depth, rows, lanes = flow_state.shape
    nx, ny, nz = counts
    half = components // 2
    per_pack = lanes // LANES
    packs = -(-components * depth // per_pack)
    devices = nx * ny * nz
    f32 = jnp.float32
    dma = pltpu.SemaphoreType.DMA
    return pl.pallas_call(
        functools.partial(kernel, counts),
        out_shape=jax.ShapeDtypeStruct((half, depth, rows, lanes), f32),
        in_specs=[pl.BlockSpec(memory_space=pl.ANY)],
        out_specs=pl.BlockSpec(memory_space=pltpu.VMEM),
        scratch_shapes=[
            pltpu.VMEM((components, depth, rows, lanes), f32),
            pltpu.VMEM((packs, rows, lanes), f32),
            pltpu.VMEM((packs, rows, lanes), f32),
            pltpu.VMEM((packs, rows, lanes), f32),
            pltpu.VMEM((components, depth, rows, lanes), f32),
            pltpu.VMEM((components, 2, rows, lanes), f32),
            pltpu.VMEM((components, 2, rows, lanes), f32),
            pltpu.VMEM((depth, rows, lanes), f32),
            pltpu.VMEM((devices, 1, lanes), f32),
            dma((2,)),
            dma((8,)),
            dma((8,)),
            dma,
            dma,
            pltpu.SemaphoreType.REGULAR,
        ],
        compiler_params=pltpu.CompilerParams(collective_id=0, has_side_effects=True, vmem_limit_bytes=VMEM_BYTES),
    )(flow_state)


def solution(mesh):
    counts = tuple(mesh.shape[axis] for axis in AXES)
    return jax.shard_map(
        functools.partial(on_device, counts),
        mesh=mesh,
        in_specs=(P(None, *AXES),),
        out_specs=P(None, *AXES),
        check_vma=False,
    )
```

```python
import functools

import jax
import jax.numpy as jnp
from jax import lax
from jax.experimental import pallas as pl
from jax.experimental.pallas import tpu as pltpu
from jax.sharding import PartitionSpec as P

MESH = pl.DeviceIdType.MESH
AXES = ("gx", "gy", "gz")
LANES = 4
VMEM_BYTES = 56281250


def shifted(values, side, dim):
    length = values.shape[dim]
    index = lax.broadcasted_iota(jnp.int32, values.shape, dim)
    return (
        pltpu.roll(jnp.where(index >= length - 2, side, values), 2, dim),
        pltpu.roll(jnp.where(index >= length - 1, side, values), 1, dim),
        pltpu.roll(jnp.where(index < 1, side, values), length - 1, dim),
        pltpu.roll(jnp.where(index < 2, side, values), length - 2, dim),
    )


def gradient(m2, m1, p1, p2):
    return (8.0 * (p1 - m1) - (p2 - m2)) * (1.0 / 12.0)


def curvature(m2, m1, center, p1, p2):
    return (16.0 * (p1 + m1) - (p2 + m2) - 30.0 * center) * (1.0 / 12.0)


def kernel(
    counts,
    flow_ref,
    out_ref,
    state,
    packed,
    from_down,
    from_up,
    beside,
    left,
    right,
    strain_ref,
    peaks,
    load_sem,
    halo_send,
    halo_recv,
    peak_send,
    peak_recv,
    ready,
):
    nx, ny, nz = counts
    components, depth, rows, lanes = state.shape
    half = components // 2
    me = [lax.axis_index(axis) for axis in AXES]

    def peer(dx, dy, dz):
        return tuple(
            lax.rem(at + (step % count), count) for at, step, count in zip(me, (dx, dy, dz), counts)
        )

    plane = [(dx, dy, 0) for dx in range(nx) for dy in range(ny) if (dx, dy) != (0, 0)]
    line = [(0, 0, dz) for dz in range(1, nz)]
    others = [(dx, dy, dz) for dz in range(1, nz) for dx in range(nx) for dy in range(ny)] + plane

    loads = [
        pltpu.make_async_copy(flow_ref.at[part], state.at[part], load_sem.at[i])
        for i, part in enumerate((pl.ds(half, half), pl.ds(0, half)))
    ]
    barrier = pltpu.get_barrier_semaphore()
    for offset in line + plane:
        pl.semaphore_signal(barrier, inc=1, device_id=peer(*offset), device_id_type=MESH)
    for load in loads:
        load.start()

    for load in loads:
        load.wait()
    tiles = [(c, x) for c in range(components) for x in range(depth)]
    per_pack = lanes // LANES
    lane = lax.broadcasted_iota(jnp.int32, (rows, lanes), 1)
    for p in range(packed.shape[0]):
        total = jnp.zeros((rows, lanes), jnp.float32)
        for t, (c, x) in enumerate(tiles[p * per_pack : (p + 1) * per_pack]):
            moved = pltpu.roll(state[c, x], (LANES * t + 2) % lanes, 1)
            total = jnp.where(lane >= LANES * t, moved, total)
        packed[p] = total

    pl.semaphore_wait(barrier, len(plane) + len(line))

    def send(i, source, target, offset):
        copy = pltpu.make_async_remote_copy(
            src_ref=source,
            dst_ref=target,
            send_sem=halo_send.at[i],
            recv_sem=halo_recv.at[i],
            device_id=peer(*offset),
            device_id_type=MESH,
        )
        copy.start()
        return copy

    velocity, vorticity = pl.ds(half, half), pl.ds(0, half)
    u_copies = [
        send(0, state.at[velocity, pl.ds(depth - 2, 2)], left.at[velocity], (1, 0, 0)),
        send(1, state.at[velocity, pl.ds(0, 2)], right.at[velocity], (-1, 0, 0)),
    ]
    near_copies = [
        send(2, packed, from_down, (0, 0, 1)),
        send(3, packed, from_up, (0, 0, -1)),
        send(4, state.at[:, :, pl.ds(rows - 8, 8)], beside.at[:, :, pl.ds(rows - 8, 8)], (0, 1, 0)),
        send(5, state.at[:, :, pl.ds(0, 8)], beside.at[:, :, pl.ds(0, 8)], (0, -1, 0)),
    ]
    for offset in plane:
        pl.semaphore_signal(ready, inc=1, device_id=peer(*offset), device_id_type=MESH)

    for copy in near_copies:
        copy.wait_recv()
    sides = [
        jnp.where((lane % LANES) < 2, from_down[p], from_up[p]) for p in range(packed.shape[0])
    ]

    def z_side(c, x):
        t = c * depth + x
        return pltpu.roll(sides[t // per_pack], (lanes - (LANES * (t % per_pack) + 2)) % lanes, 1)

    for x in range(depth):
        strain = jnp.zeros((rows, lanes), jnp.float32)
        w_y, w_z = state[1, x], state[2, x]
        for c in range(half):
            u = state[half + c, x]
            grad_y = gradient(*shifted(u, beside[half + c, x], 0))
            grad_z = gradient(*shifted(u, z_side(half + c, x), 1))
            strain = strain + grad_y * grad_y + grad_z * grad_z
            out_ref[c, x] = w_y * grad_y + w_z * grad_z
        strain_ref[x] = strain

    def layer(c, x):
        if x < 0:
            return left[c, x + 2]
        if x >= depth:
            return right[c, x - depth]
        return state[c, x]

    for copy in u_copies:
        copy.wait_recv()
    peak = jnp.zeros((rows, lanes), jnp.float32)
    for x in range(depth):
        strain = strain_ref[x]
        w_x = state[0, x]
        for c in range(half):
            grad_x = gradient(*(layer(half + c, x + k) for k in (-2, -1, 1, 2)))
            strain = strain + grad_x * grad_x
            out_ref[c, x] = out_ref[c, x] + w_x * grad_x
        peak = jnp.maximum(peak, strain)

    peaks[0] = jnp.max(peak, axis=0, keepdims=True)
    pl.semaphore_wait(ready, len(plane))
    peak_copies = []
    for i, offset in enumerate(others):
        copy = pltpu.make_async_remote_copy(
            src_ref=peaks.at[0],
            dst_ref=peaks.at[i + 1],
            send_sem=peak_send,
            recv_sem=peak_recv,
            device_id=peer(*offset),
            device_id_type=MESH,
        )
        copy.start()
        peak_copies.append(copy)
    w_copies = [
        send(6, state.at[vorticity, pl.ds(depth - 2, 2)], left.at[vorticity], (1, 0, 0)),
        send(7, state.at[vorticity, pl.ds(0, 2)], right.at[vorticity], (-1, 0, 0)),
    ]
    for copy in w_copies:
        copy.wait_recv()
    for x in range(depth):
        for c in range(half):
            m2, m1, w, p1, p2 = (layer(c, x + k) for k in (-2, -1, 0, 1, 2))
            laplace = curvature(m2, m1, w, p1, p2)
            m2, m1, p1, p2 = shifted(w, beside[c, x], 0)
            laplace = laplace + curvature(m2, m1, w, p1, p2)
            m2, m1, p1, p2 = shifted(w, z_side(c, x), 1)
            laplace = laplace + curvature(m2, m1, w, p1, p2)
            out_ref[c, x] = out_ref[c, x] + 0.5 * laplace
    pltpu.make_async_copy(peaks.at[pl.ds(1, len(others))], peaks.at[pl.ds(1, len(others))], peak_send).wait()
    for copy in u_copies + near_copies + w_copies:
        copy.wait_send()
    everyone = pltpu.make_async_copy(peaks.at[pl.ds(1, len(others))], peaks.at[pl.ds(1, len(others))], peak_recv)
    everyone.wait()
    peak = jnp.max(jnp.max(peaks[...], axis=0), axis=1, keepdims=True)
    step_size = 0.25 / jnp.maximum(1.0, jnp.sqrt(peak))
    for x in range(depth):
        for c in range(half):
            out_ref[c, x] = state[c, x] + step_size * out_ref[c, x]


def on_device(counts, flow_state):
    components, depth, rows, lanes = flow_state.shape
    nx, ny, nz = counts
    half = components // 2
    per_pack = lanes // LANES
    packs = -(-components * depth // per_pack)
    devices = nx * ny * nz
    f32 = jnp.float32
    dma = pltpu.SemaphoreType.DMA
    return pl.pallas_call(
        functools.partial(kernel, counts),
        out_shape=jax.ShapeDtypeStruct((half, depth, rows, lanes), f32),
        in_specs=[pl.BlockSpec(memory_space=pl.ANY)],
        out_specs=pl.BlockSpec(memory_space=pltpu.VMEM),
        scratch_shapes=[
            pltpu.VMEM((components, depth, rows, lanes), f32),
            pltpu.VMEM((packs, rows, lanes), f32),
            pltpu.VMEM((packs, rows, lanes), f32),
            pltpu.VMEM((packs, rows, lanes), f32),
            pltpu.VMEM((components, depth, rows, lanes), f32),
            pltpu.VMEM((components, 2, rows, lanes), f32),
            pltpu.VMEM((components, 2, rows, lanes), f32),
            pltpu.VMEM((depth, rows, lanes), f32),
            pltpu.VMEM((devices, 1, lanes), f32),
            dma((2,)),
            dma((8,)),
            dma((8,)),
            dma,
            dma,
            pltpu.SemaphoreType.REGULAR,
        ],
        compiler_params=pltpu.CompilerParams(collective_id=0, has_side_effects=True, vmem_limit_bytes=VMEM_BYTES),
    )(flow_state)


def solution(mesh):
    counts = tuple(mesh.shape[axis] for axis in AXES)
    return jax.shard_map(
        functools.partial(on_device, counts),
        mesh=mesh,
        in_specs=(P(None, *AXES),),
        out_specs=P(None, *AXES),
        check_vma=False,
    )
```

```python
import functools

import jax
import jax.numpy as jnp
from jax import lax
from jax.experimental import pallas as pl
from jax.experimental.pallas import tpu as pltpu
from jax.sharding import PartitionSpec as P

MESH = pl.DeviceIdType.MESH
AXES = ("gx", "gy", "gz")
LANES = 4
VMEM_BYTES = 56281250


def shifted(values, side, dim):
    length = values.shape[dim]
    index = lax.broadcasted_iota(jnp.int32, values.shape, dim)
    return (
        pltpu.roll(jnp.where(index >= length - 2, side, values), 2, dim),
        pltpu.roll(jnp.where(index >= length - 1, side, values), 1, dim),
        pltpu.roll(jnp.where(index < 1, side, values), length - 1, dim),
        pltpu.roll(jnp.where(index < 2, side, values), length - 2, dim),
    )


def gradient(m2, m1, p1, p2):
    return (8.0 * (p1 - m1) - (p2 - m2)) * (1.0 / 12.0)


def curvature(m2, m1, center, p1, p2):
    return (16.0 * (p1 + m1) - (p2 + m2) - 30.0 * center) * (1.0 / 12.0)


def kernel(
    counts,
    flow_ref,
    out_ref,
    state,
    packed,
    from_down,
    from_up,
    beside,
    left,
    right,
    strain_ref,
    peaks,
    load_sem,
    halo_send,
    halo_recv,
    peak_send,
    peak_recv,
    ready,
):
    nx, ny, nz = counts
    components, depth, rows, lanes = state.shape
    half = components // 2
    me = [lax.axis_index(axis) for axis in AXES]

    def peer(dx, dy, dz):
        return tuple(
            lax.rem(at + (step % count), count) for at, step, count in zip(me, (dx, dy, dz), counts)
        )

    plane = [(dx, dy, 0) for dx in range(nx) for dy in range(ny) if (dx, dy) != (0, 0)]
    line = [(0, 0, dz) for dz in range(1, nz)]
    others = [(dx, dy, dz) for dz in range(1, nz) for dx in range(nx) for dy in range(ny)] + plane

    loads = [
        pltpu.make_async_copy(flow_ref.at[part], state.at[part], load_sem.at[i])
        for i, part in enumerate((pl.ds(half, half), pl.ds(0, half)))
    ]
    barrier = pltpu.get_barrier_semaphore()
    for offset in line + plane:
        pl.semaphore_signal(barrier, inc=1, device_id=peer(*offset), device_id_type=MESH)
    for load in loads:
        load.start()

    for load in loads:
        load.wait()
    tiles = [(c, x) for c in range(components) for x in range(depth)]
    per_pack = lanes // LANES
    lane = lax.broadcasted_iota(jnp.int32, (rows, lanes), 1)
    for p in range(packed.shape[0]):
        total = jnp.zeros((rows, lanes), jnp.float32)
        for t, (c, x) in enumerate(tiles[p * per_pack : (p + 1) * per_pack]):
            moved = pltpu.roll(state[c, x], (LANES * t + 2) % lanes, 1)
            total = jnp.where(lane >= LANES * t, moved, total)
        packed[p] = total

    pl.semaphore_wait(barrier, len(plane) + len(line))

    def send(i, source, target, offset):
        copy = pltpu.make_async_remote_copy(
            src_ref=source,
            dst_ref=target,
            send_sem=halo_send.at[i],
            recv_sem=halo_recv.at[i],
            device_id=peer(*offset),
            device_id_type=MESH,
        )
        copy.start()
        return copy

    velocity, vorticity = pl.ds(half, half), pl.ds(0, half)
    u_copies = [
        send(0, state.at[velocity, pl.ds(depth - 2, 2)], left.at[velocity], (1, 0, 0)),
        send(1, state.at[velocity, pl.ds(0, 2)], right.at[velocity], (-1, 0, 0)),
    ]
    near_copies = [
        send(2, packed, from_down, (0, 0, 1)),
        send(3, packed, from_up, (0, 0, -1)),
        send(4, state.at[:, :, pl.ds(rows - 8, 8)], beside.at[:, :, pl.ds(rows - 8, 8)], (0, 1, 0)),
        send(5, state.at[:, :, pl.ds(0, 8)], beside.at[:, :, pl.ds(0, 8)], (0, -1, 0)),
    ]
    for offset in plane:
        pl.semaphore_signal(ready, inc=1, device_id=peer(*offset), device_id_type=MESH)

    for copy in near_copies:
        copy.wait_recv()
    sides = [
        jnp.where((lane % LANES) < 2, from_down[p], from_up[p]) for p in range(packed.shape[0])
    ]

    def z_side(c, x):
        t = c * depth + x
        return pltpu.roll(sides[t // per_pack], (lanes - (LANES * (t % per_pack) + 2)) % lanes, 1)

    for x in range(depth):
        strain = jnp.zeros((rows, lanes), jnp.float32)
        w_y, w_z = state[1, x], state[2, x]
        for c in range(half):
            u = state[half + c, x]
            grad_y = gradient(*shifted(u, beside[half + c, x], 0))
            grad_z = gradient(*shifted(u, z_side(half + c, x), 1))
            strain = strain + grad_y * grad_y + grad_z * grad_z
            out_ref[c, x] = w_y * grad_y + w_z * grad_z
        strain_ref[x] = strain

    def layer(c, x):
        if x < 0:
            return left[c, x + 2]
        if x >= depth:
            return right[c, x - depth]
        return state[c, x]

    for copy in u_copies:
        copy.wait_recv()
    w_copies = [
        send(6, state.at[vorticity, pl.ds(depth - 2, 2)], left.at[vorticity], (1, 0, 0)),
        send(7, state.at[vorticity, pl.ds(0, 2)], right.at[vorticity], (-1, 0, 0)),
    ]
    peak = jnp.zeros((rows, lanes), jnp.float32)
    for x in range(depth):
        strain = strain_ref[x]
        w_x = state[0, x]
        for c in range(half):
            grad_x = gradient(*(layer(half + c, x + k) for k in (-2, -1, 1, 2)))
            strain = strain + grad_x * grad_x
            out_ref[c, x] = out_ref[c, x] + w_x * grad_x
        peak = jnp.maximum(peak, strain)

    peaks[0] = jnp.max(peak, axis=0, keepdims=True)
    pl.semaphore_wait(ready, len(plane))
    peak_copies = []
    for i, offset in enumerate(others):
        copy = pltpu.make_async_remote_copy(
            src_ref=peaks.at[0],
            dst_ref=peaks.at[i + 1],
            send_sem=peak_send,
            recv_sem=peak_recv,
            device_id=peer(*offset),
            device_id_type=MESH,
        )
        copy.start()
        peak_copies.append(copy)
    for copy in w_copies:
        copy.wait_recv()
    for x in range(depth):
        for c in range(half):
            m2, m1, w, p1, p2 = (layer(c, x + k) for k in (-2, -1, 0, 1, 2))
            laplace = curvature(m2, m1, w, p1, p2)
            m2, m1, p1, p2 = shifted(w, beside[c, x], 0)
            laplace = laplace + curvature(m2, m1, w, p1, p2)
            m2, m1, p1, p2 = shifted(w, z_side(c, x), 1)
            laplace = laplace + curvature(m2, m1, w, p1, p2)
            out_ref[c, x] = out_ref[c, x] + 0.5 * laplace
    pltpu.make_async_copy(peaks.at[pl.ds(1, len(others))], peaks.at[pl.ds(1, len(others))], peak_send).wait()
    for copy in u_copies + near_copies + w_copies:
        copy.wait_send()
    everyone = pltpu.make_async_copy(peaks.at[pl.ds(1, len(others))], peaks.at[pl.ds(1, len(others))], peak_recv)
    everyone.wait()
    peak = jnp.max(jnp.max(peaks[...], axis=0), axis=1, keepdims=True)
    step_size = 0.25 / jnp.maximum(1.0, jnp.sqrt(peak))
    for x in range(depth):
        for c in range(half):
            out_ref[c, x] = state[c, x] + step_size * out_ref[c, x]


def on_device(counts, flow_state):
    components, depth, rows, lanes = flow_state.shape
    nx, ny, nz = counts
    half = components // 2
    per_pack = lanes // LANES
    packs = -(-components * depth // per_pack)
    devices = nx * ny * nz
    f32 = jnp.float32
    dma = pltpu.SemaphoreType.DMA
    return pl.pallas_call(
        functools.partial(kernel, counts),
        out_shape=jax.ShapeDtypeStruct((half, depth, rows, lanes), f32),
        in_specs=[pl.BlockSpec(memory_space=pl.ANY)],
        out_specs=pl.BlockSpec(memory_space=pltpu.VMEM),
        scratch_shapes=[
            pltpu.VMEM((components, depth, rows, lanes), f32),
            pltpu.VMEM((packs, rows, lanes), f32),
            pltpu.VMEM((packs, rows, lanes), f32),
            pltpu.VMEM((packs, rows, lanes), f32),
            pltpu.VMEM((components, depth, rows, lanes), f32),
            pltpu.VMEM((components, 2, rows, lanes), f32),
            pltpu.VMEM((components, 2, rows, lanes), f32),
            pltpu.VMEM((depth, rows, lanes), f32),
            pltpu.VMEM((devices, 1, lanes), f32),
            dma((2,)),
            dma((8,)),
            dma((8,)),
            dma,
            dma,
            pltpu.SemaphoreType.REGULAR,
        ],
        compiler_params=pltpu.CompilerParams(collective_id=0, has_side_effects=True, vmem_limit_bytes=VMEM_BYTES),
    )(flow_state)


def solution(mesh):
    counts = tuple(mesh.shape[axis] for axis in AXES)
    return jax.shard_map(
        functools.partial(on_device, counts),
        mesh=mesh,
        in_specs=(P(None, *AXES),),
        out_specs=P(None, *AXES),
        check_vma=False,
    )
```
